32 devices in a mesh: ep: 16 (over z, y, x), dp: 2 (over core).
Axes of the slice: x: 2, y: 2, z: 4, core: 2. Of those that a mesh axis runs over, the one named last changes fastest.
Arguments:
- grad_out: bfloat16 [4096, 2048], P(('ep', 'dp')), may hold values from -6 to 6
- router_prob: bfloat16 [4096], P(('ep', 'dp')), may hold values from 0.19921875 to 1
- routes: int32 [4096, 1], P(('ep', 'dp')), may hold values from 0 to 63, as said below
- token_inputs: bfloat16 [4096, 2048], P(('ep', 'dp')), may hold values from -6 to 6
- w_in: bfloat16 [7168, 2048], P(('ep', 'dp')), may hold values from -0.125 to 0.125
- w_out: bfloat16 [7168, 2048], P(('ep', 'dp')), may hold values from -0.0625 to 0.0625
Outputs:
- grad_tokens: bfloat16 [4096, 2048], P(('ep', 'dp'))
- grad_in_weight: bfloat16 [7168, 2048], P(('ep', 'dp'))
- grad_out_weight: bfloat16 [7168, 2048], P(('ep', 'dp'))
The draws below stay inside these ranges and needn't reach their ends.
Inputs may be any that keep to these rules, and one draw needn't show every extreme that they name: `routes`: ids below 1 are the experts of this window; the rows of one device name each of them at most 3 times, and in every draw one of them is named exactly 3 times by the rows of every device of one dp index.
All inputs are finite; a program needn't handle non-finite values.
Results may differ from the reference program's by a relative error of at most 0.014.
Values may be sent and summed in bfloat16 or wider, within the bound.
No kernel may reach another device: no remote copies, remote signals or barrier semaphores. Data moves between devices by JAX's collectives and lax.ppermute only.
A program may use at most 64 MiB of HBM per device.

```python
import math
import jax
import jax.numpy as jnp
from jax import lax

D = 2048
EXPERT_FF = 7168
EXPERTS = 64
GROUP = 16
CAP = 3
TOK_DEV = 128
FLIGHT = 1
SLOTS = 48
REPLICAS = 2
TOKENS = 4096


def shuffle_row(row_key, row_values):
    return jax.random.permutation(row_key, row_values)


def draw_routes(key, part):
    blocks = TOKENS // TOK_DEV
    key_count, key_hot, key_other, key_order = jax.random.split(key, 4)
    counts = jax.random.randint(key_count, (blocks, FLIGHT), 0, CAP + 1)
    hot_rows = jax.random.randint(key_hot, (REPLICAS,), 0, FLIGHT)
    block_ids = jnp.arange(blocks, dtype=jnp.int32)
    hottest = hot_rows[block_ids % REPLICAS]
    counts = jnp.where(jnp.arange(FLIGHT, dtype=jnp.int32)[None, :] == hottest[:, None], CAP, counts)
    bounds = jnp.cumsum(counts, axis=1)
    position = jnp.arange(TOK_DEV, dtype=jnp.int32)
    chosen = jnp.sum((position[None, :, None] >= bounds[:, None, :]).astype(jnp.int32), axis=2)
    others = FLIGHT + jax.random.randint(key_other, (blocks, TOK_DEV), 0, EXPERTS - FLIGHT)
    chosen = jnp.where(chosen < FLIGHT, chosen, others)
    order_keys = jax.random.split(key_order, blocks)
    shuffled = jax.vmap(shuffle_row)(order_keys, chosen)
    return shuffled.reshape(TOKENS, 1).astype(jnp.int32)


def block_levels(key, shape, pieces, low, largest):
    def one(axis_at, shards_of):
        draws = jax.random.uniform(jax.random.fold_in(jax.random.fold_in(key, 6), axis_at), (shards_of,), jnp.float32, low / len(pieces), largest / len(pieces))
        return jnp.repeat(jnp.exp(draws), shape[axis_at] // shards_of).reshape((-1,) + (1,) * (len(shape) - axis_at - 1))

    loudness = one(*pieces[0])
    for cut in pieces[1:]:
        loudness = loudness * one(*cut)
    return loudness


def noise(key, extent, spread, bound, cuts=(), held_as=jnp.bfloat16):
    drawn = jax.random.normal(key, extent, jnp.float32) * spread
    if len(cuts) > 0:
        drawn = block_levels(key, extent, cuts, -0.22, 0.18) * drawn
    return jnp.clip(drawn, min=-bound, max=bound).astype(held_as)


def setup_inputs(seed: int = 0) -> dict:
    key_of = jax.random.split(jax.random.key(seed), 7)
    grad_out = noise(key_of[0], (TOKENS, D), 1.0, 6.0, ((0, 32),))
    router_prob = jnp.clip(0.19921875 + 0.80078125 * jax.random.uniform(key_of[1], (TOKENS,), jnp.float32) ** block_levels(key_of[1], (TOKENS,), ((0, 32),), -0.2, 0.2), 0.19921875, 1.0).astype(jnp.bfloat16)
    routes = draw_routes(jax.random.fold_in(key_of[6], 71), 0)
    token_inputs = noise(key_of[3], (TOKENS, D), 1.0, 6.0, ((0, 32),))
    w_in = noise(key_of[4], (FLIGHT * EXPERT_FF, D), D ** -0.5, 0.125, ((0, 32),))
    w_out = noise(key_of[5], (FLIGHT * EXPERT_FF, D), EXPERT_FF ** -0.5, 0.0625, ((0, 32),))
    return {"grad_out": grad_out, "router_prob": router_prob, "routes": routes, "token_inputs": token_inputs, "w_in": w_in, "w_out": w_out}


def slot_rows(routes):
    blocks = TOKENS // TOK_DEV
    chosen = routes[:, 0].reshape(blocks, TOK_DEV)
    onehot = (chosen[:, :, None] == jnp.arange(FLIGHT, dtype=jnp.int32)[None, None, :]).astype(jnp.int32)
    before = jnp.cumsum(onehot, axis=1) - onehot
    slot_rank = lax.optimization_barrier(jnp.sum(before * onehot, axis=2))
    block_ids = jnp.arange(blocks, dtype=jnp.int32)[:, None]
    source = block_ids // REPLICAS
    replica = block_ids % REPLICAS
    in_window = chosen < FLIGHT
    dest_rows = (chosen * REPLICAS + replica) * SLOTS + source * CAP + slot_rank
    all_rows = FLIGHT * REPLICAS * SLOTS
    dest_rows = jnp.where(in_window, dest_rows, all_rows)
    return (dest_rows.reshape(-1).astype(jnp.int32), in_window.reshape(-1))

def reference(grad_out, router_prob, routes, token_inputs, w_in, w_out):
    dest_rows, in_window = slot_rows(routes)
    all_rows = FLIGHT * REPLICAS * SLOTS
    scaled = (router_prob.astype(jnp.float32)[:, None] * grad_out.astype(jnp.float32)).astype(jnp.bfloat16)
    dispatched = jnp.zeros((all_rows, D), jnp.bfloat16).at[dest_rows].set(scaled, mode='drop')
    gathered_inputs = jnp.zeros((all_rows, D), jnp.bfloat16).at[dest_rows].set(token_inputs, mode='drop')
    group_inputs = gathered_inputs.reshape(FLIGHT, REPLICAS, SLOTS, D)
    group_grads = dispatched.reshape(FLIGHT, REPLICAS, SLOTS, D)
    weights_in = w_in.reshape(FLIGHT, EXPERT_FF, D)
    weights_out = w_out.reshape(FLIGHT, EXPERT_FF, D)
    grad_scale = 1.0 / math.sqrt(REPLICAS * SLOTS)
    piece_size = EXPERT_FF // GROUP

    def one_expert(operands):
        inputs, slot_grads, weight_in, weight_out = operands
        weight_pieces = weight_in.reshape(GROUP, piece_size, D)

        def one_replica(pair):
            rows_in, cotangent = pair
            pre_act = jnp.dot(rows_in, weight_in.T, preferred_element_type=jnp.float32)
            gate_sig = jax.nn.sigmoid(pre_act)
            hidden = (pre_act * gate_sig).astype(jnp.bfloat16)
            back_prop = jnp.dot(cotangent, weight_out.T, preferred_element_type=jnp.float32)
            grad_pre = (back_prop * gate_sig * (1.0 + pre_act * (1.0 - gate_sig))).astype(jnp.bfloat16)
            grad_pieces = jnp.transpose(grad_pre.reshape(SLOTS, GROUP, piece_size), (1, 0, 2))

            def add_piece(total, items):
                grad_piece, weight_piece = items
                piece_grad = jnp.dot(grad_piece, weight_piece, preferred_element_type=jnp.float32).astype(jnp.bfloat16)
                piece_grad = lax.optimization_barrier(piece_grad).astype(jnp.float32)
                return (total + piece_grad, None)
            slot_grad, unused = lax.scan(add_piece, jnp.zeros((SLOTS, D), jnp.float32), (grad_pieces, weight_pieces))
            part_in = jnp.dot(grad_pre.T, rows_in, preferred_element_type=jnp.float32).astype(jnp.bfloat16)
            part_out = jnp.dot(hidden.T, cotangent, preferred_element_type=jnp.float32).astype(jnp.bfloat16)
            part_in = lax.optimization_barrier(part_in).astype(jnp.float32)
            part_out = lax.optimization_barrier(part_out).astype(jnp.float32)
            return (slot_grad, part_in, part_out)
        slot_grad, part_in, part_out = lax.map(one_replica, (inputs, slot_grads))
        grad_in = (lax.optimization_barrier(jnp.sum(part_in, axis=0)) * grad_scale).astype(jnp.bfloat16)
        grad_outw = (lax.optimization_barrier(jnp.sum(part_out, axis=0)) * grad_scale).astype(jnp.bfloat16)
        return (slot_grad, grad_in, grad_outw)
    slot_grad, grad_in, grad_outw = lax.map(one_expert, (group_inputs, group_grads, weights_in, weights_out))
    flat_grad = slot_grad.reshape(all_rows, D)
    picked = flat_grad[jnp.minimum(dest_rows, all_rows - 1).astype(jnp.int32)]
    grad_tokens = jnp.where(in_window[:, None], picked, jnp.float32(0.0)).astype(jnp.bfloat16)
    return (grad_tokens, grad_in.reshape(FLIGHT * EXPERT_FF, D), grad_outw.reshape(FLIGHT * EXPERT_FF, D))
```

```python
import functools
import math

import jax
import jax.numpy as jnp
from jax import lax
from jax.experimental import pallas as pl
from jax.experimental.pallas import tpu as pltpu
from jax.sharding import PartitionSpec as P

GROUP = 16
CAP = 3


BF16 = jnp.bfloat16
F32 = jnp.float32
VM = pl.BlockSpec(memory_space=pltpu.VMEM)
NT = (((1,), (1,)), ((), ()))
NN = (((1,), (0,)), ((), ()))
TN = (((0,), (0,)), ((), ()))


def dot(a, b, dims):
    return lax.dot_general(a, b, dims, preferred_element_type=F32)


def call(body, outs, *args, flops=1 << 20, in_specs=None, out_specs=None, grid=()):
    return pl.pallas_call(
        body,
        out_shape=outs,
        grid=grid,
        in_specs=in_specs or [VM] * len(args),
        out_specs=out_specs or jax.tree.map(lambda _: VM, outs),
        cost_estimate=pl.CostEstimate(flops=flops, bytes_accessed=1 << 16, transcendentals=0),
    )(*args)


def slot_choice(routes_row, rows, base):
    tokens = routes_row.shape[1]
    inside = (routes_row < 1).astype(F32)
    u = lax.broadcasted_iota(jnp.int32, (tokens, tokens), 0)
    t = lax.broadcasted_iota(jnp.int32, (tokens, tokens), 1)
    earlier = (u < t).astype(BF16)
    inside_rows = jnp.broadcast_to(inside, (8, tokens)).astype(BF16)
    rank = dot(inside_rows, earlier, NN)
    slot = lax.broadcasted_iota(jnp.int32, (rows, tokens), 0).astype(F32) - base
    valid = (slot >= 0) & (slot < CAP)
    return jnp.where(valid & (rank[:1] == slot) & (routes_row < 1), 1.0, 0.0)


def pack_kernel(routes_ref, prob_ref, grad_ref, tok_ref, out_ref):
    routes = routes_ref[...]
    pick_q = slot_choice(routes, 8, 0)
    pick_x = slot_choice(routes, 8, CAP)
    prob = jnp.sum(pick_q * prob_ref[...].astype(F32), axis=1, keepdims=True)
    q = dot(pick_q.astype(BF16), grad_ref[...], NN) * prob
    x = dot(pick_x.astype(BF16), tok_ref[...], NN)
    out_ref[...] = (q + x).astype(BF16)


def join_kernel(count, *refs):
    out_ref = refs[-1]
    rows = [r[...].astype(F32)[: 2 * CAP] for r in refs[:count]]
    out_ref[...] = jnp.concatenate(rows, axis=0).astype(BF16)


def hidden_part(a, w_in, w_out, gin_ref, hid_ref):
    n = a.shape[0]
    pre_x = dot(w_in, a, NT)
    back = dot(w_out, a, NT)
    col = lax.broadcasted_iota(jnp.int32, pre_x.shape, 1)
    is_q = lax.rem(col, 2 * CAP) < CAP
    pre = jnp.where(is_q, pltpu.roll(pre_x, n - CAP, 1), 0.0) if n % 128 == 0 else jnp.where(
        is_q, jnp.concatenate([pre_x[:, CAP:], pre_x[:, :CAP]], axis=1), 0.0
    )
    sig = jax.nn.sigmoid(pre)
    hid = jnp.where(is_q, pre * sig, 0.0).astype(BF16)
    gpre = jnp.where(is_q, back * sig * (1.0 + pre * (1.0 - sig)), 0.0)
    hid_ref[...] = hid
    gin_ref[...] = jnp.concatenate([gpre[:, n - CAP :], gpre[:, : n - CAP]], axis=1).astype(BF16)
    return gpre.astype(BF16)


def compact(gpre, pad, per):
    n = gpre.shape[1]
    blocks = n // (2 * per)
    r = lax.broadcasted_iota(jnp.int32, (blocks * pad, n), 0)
    c = lax.broadcasted_iota(jnp.int32, (blocks * pad, n), 1)
    inner = lax.rem(r, pad)
    src = lax.div(r, pad) * (2 * per) + lax.div(inner, CAP) * (2 * CAP) + lax.rem(inner, CAP)
    sel = jnp.where((c == src) & (inner < per), 1.0, 0.0).astype(BF16)
    return dot(sel, gpre, NT).astype(BF16)


def middle_kernel(pad, per, a_ref, w_in_ref, w_out_ref, gin_ref, hid_ref, part_ref):
    w_in = w_in_ref[...]
    gpre = hidden_part(a_ref[...], w_in, w_out_ref[...], gin_ref, hid_ref)
    part_ref[...] = dot(compact(gpre, pad, per), w_in, NN).astype(part_ref.dtype)


def weight_kernel(scale, l0_ref, l1_ref, a0_ref, a1_ref, out_ref):
    left = jnp.concatenate([l0_ref[...], l1_ref[...]], axis=1)
    right = jnp.concatenate([a0_ref[...], a1_ref[...]], axis=0)
    out_ref[...] = (dot(left, right, NN) * scale).astype(BF16)


def add_kernel(a_ref, b_ref, out_ref):
    out_ref[...] = (a_ref[...].astype(F32) + b_ref[...].astype(F32)).astype(BF16)


def sum_kernel(count, per, *refs):
    out_refs = refs[count:]
    total = refs[0][...].astype(F32)
    for r in refs[1:count]:
        total = total + r[...].astype(F32)
    for i, out in enumerate(out_refs):
        out[...] = jnp.concatenate(
            [total[i * CAP : (i + 1) * CAP], jnp.zeros((8 - CAP, total.shape[1]), F32)], axis=0
        ).astype(out.dtype)


def final_kernel(count, *refs):
    routes_ref, out_ref = refs[count], refs[count + 1]
    total = refs[0][...].astype(F32)
    for r in refs[1:count]:
        total = total + r[...].astype(F32)
    pick = slot_choice(routes_ref[...], 8, 0).astype(BF16)
    out_ref[...] = dot(pick, total.astype(BF16), TN).astype(BF16)


def xor_swap(x, axis, k):
    n = lax.axis_size(axis)
    return lax.ppermute(x, axis, [(i, i ^ k) for i in range(n)])


def one_expert(grad_out, router_prob, routes, token_inputs, w_in, w_out):
    ep_count = lax.axis_size("ep")
    replicas = lax.axis_size("dp")
    tokens, width = grad_out.shape
    hidden = w_in.shape[0]
    inner = 1 << (int(math.log2(ep_count)) // 2)
    outer = ep_count // inner
    near = [1, 2, 3] if inner == 4 else list(range(1, inner))
    far = [k * inner for k in range(1, outer)]
    sds = jax.ShapeDtypeStruct
    routes_row = routes.reshape(1, tokens)
    prob_row = router_prob.reshape(1, tokens)

    own = call(pack_kernel, sds((8, width), BF16), routes_row, prob_row, grad_out, token_inputs)
    blocks = [own] + [xor_swap(own, "ep", k) for k in far]
    column = call(
        functools.partial(join_kernel, outer), sds((2 * CAP * outer, width), BF16), *blocks
    )
    mine = jnp.concatenate([column] + [xor_swap(column, "ep", k) for k in near], axis=0)
    other = xor_swap(mine, "dp", 1)

    per = CAP * outer
    pad = -(-per // 8) * 8
    rows = mine.shape[0]
    half_flops = 6 * rows * hidden * width
    parts = {}
    for name, a, dt in (("mine", mine, F32), ("other", other, BF16)):
        parts[name] = call(
            functools.partial(middle_kernel, pad, per),
            (sds((hidden, rows), BF16), sds((hidden, rows), BF16), sds((inner * pad, width), dt)),
            a,
            w_in,
            w_out,
            flops=half_flops,
        )
    back = xor_swap(parts["other"][2], "dp", 1)
    piece = call(add_kernel, sds((inner * pad, width), BF16), parts["mine"][2], back)
    piece = piece.reshape(inner, pad, width)
    slots = [piece[0]] + [xor_swap(piece[i + 1], "ep", k) for i, k in enumerate(near)]
    rows8 = call(
        functools.partial(sum_kernel, inner, per),
        tuple(sds((8, width), F32 if i == 0 else BF16) for i in range(outer)),
        *slots,
    )
    last = [rows8[0]] + [xor_swap(rows8[i + 1], "ep", k) for i, k in enumerate(far)]
    grad_tokens = call(
        functools.partial(final_kernel, outer), sds((tokens, width), BF16), *last, routes_row
    )

    scale = 1.0 / math.sqrt(replicas * ep_count * CAP)
    grads = []
    cut = width // 4
    for i in (0, 1):
        other_i = i
        l0, l1 = parts["mine"][i], parts["other"][other_i]
        grads.append(
            call(
                functools.partial(weight_kernel, scale),
                sds((hidden, width), BF16),
                l0,
                l1,
                mine,
                other,
                grid=(width // cut,),
                in_specs=[
                    VM,
                    VM,
                    pl.BlockSpec((rows, cut), lambda c: (0, c)),
                    pl.BlockSpec((rows, cut), lambda c: (0, c)),
                ],
                out_specs=pl.BlockSpec((hidden, cut), lambda c: (0, c)),
                flops=4 * rows * hidden * width,
            )
        )
    return grad_tokens, grads[0], grads[1]


def per_device(grad_out, router_prob, routes, token_inputs, w_in, w_out):
    ep_count = lax.axis_size("ep")
    replicas = lax.axis_size("dp")
    flight = ep_count // GROUP
    if flight == 1 and replicas == 2:
        return one_expert(grad_out, router_prob, routes, token_inputs, w_in, w_out)
    tok_rows = grad_out.shape[0]
    model_width = grad_out.shape[1]
    expert_ids = routes[:, 0]
    in_window = expert_ids < flight
    onehot = (expert_ids[:, None] == jnp.arange(flight, dtype=jnp.int32)[None, :]).astype(
        jnp.bfloat16
    )
    earlier = (
        jnp.arange(tok_rows, dtype=jnp.int32)[:, None]
        > jnp.arange(tok_rows, dtype=jnp.int32)[None, :]
    ).astype(jnp.bfloat16)
    before = jnp.dot(earlier, onehot, preferred_element_type=jnp.float32)
    slot_rank = jnp.sum(before * onehot.astype(jnp.float32), axis=1).astype(jnp.int32)
    window_rows = flight * CAP
    target = jnp.where(in_window, expert_ids * CAP + slot_rank, window_rows)
    chooser = (jnp.arange(window_rows, dtype=jnp.int32)[:, None] == target[None, :]).astype(
        jnp.bfloat16
    )
    scaled = (router_prob.astype(jnp.float32)[:, None] * grad_out.astype(jnp.float32)).astype(
        jnp.bfloat16
    )
    paired = jnp.concatenate((scaled, token_inputs), axis=1)
    outgoing = jnp.dot(chooser, paired, preferred_element_type=jnp.float32).astype(jnp.bfloat16)
    outgoing = jnp.broadcast_to(
        outgoing.reshape(flight, 1, CAP, 2 * model_width), (flight, GROUP, CAP, 2 * model_width)
    )
    outgoing = outgoing.reshape(ep_count, CAP, 2 * model_width)
    incoming = lax.all_to_all(outgoing, "ep", split_axis=0, concat_axis=0, tiled=True)
    slot_total = ep_count * CAP
    incoming = incoming.reshape(slot_total, 2 * model_width)
    cotangent = incoming[:, :model_width]
    rows_in = incoming[:, model_width:]
    weight_in, weight_out = (
        lax.all_gather(w_in, "dp", axis=0, tiled=True),
        lax.all_gather(w_out, "dp", axis=0, tiled=True),
    )
    contract_last = (((1,), (1,)), ((), ()))
    contract_first = (((0,), (0,)), ((), ()))
    pre_act = lax.dot_general(rows_in, weight_in, contract_last, preferred_element_type=jnp.float32)
    gate_sig = jax.nn.sigmoid(pre_act)
    hidden = (pre_act * gate_sig).astype(jnp.bfloat16)
    back_prop = lax.dot_general(
        cotangent, weight_out, contract_last, preferred_element_type=jnp.float32
    )
    grad_pre = (back_prop * gate_sig * (1.0 + pre_act * (1.0 - gate_sig))).astype(jnp.bfloat16)
    piece_grad = jnp.dot(grad_pre, weight_in, preferred_element_type=jnp.float32).astype(
        jnp.bfloat16
    )
    piece_grad = piece_grad.reshape(ep_count, CAP, model_width)
    returned = lax.all_to_all(piece_grad, "ep", split_axis=0, concat_axis=0, tiled=True)
    summed = jnp.sum(returned.reshape(flight, GROUP, CAP, model_width).astype(jnp.float32), axis=1)
    summed = summed.reshape(window_rows, model_width)
    picked = jnp.take(summed, jnp.minimum(target, window_rows - 1), axis=0)
    grad_tokens = jnp.where(in_window[:, None], picked, jnp.float32(0.0)).astype(jnp.bfloat16)
    grad_scale = 1.0 / math.sqrt(replicas * slot_total)
    grads = []
    for columns, rows in ((grad_pre, rows_in), (hidden, cotangent)):
        part = lax.dot_general(columns, rows, contract_first, preferred_element_type=jnp.float32)
        total = lax.psum_scatter(part.astype(jnp.bfloat16), "dp", scatter_dimension=0, tiled=True)
        grads.append((total.astype(jnp.float32) * grad_scale).astype(jnp.bfloat16))
    return grad_tokens, grads[0], grads[1]


def solution(mesh):
    spec = P(("ep", "dp"), None)
    in_specs = (spec, P(("ep", "dp")), spec, spec, spec, spec)
    return jax.shard_map(
        per_device, mesh=mesh, in_specs=in_specs, out_specs=(spec,) * 3, check_vma=False
    )
```
